32 devices in a mesh: grp: 2 (over core), tab: 16 (over z, y, x).
Axes of the slice: x: 2, y: 2, z: 4, core: 2. Of those that a mesh axis runs over, the one named last changes fastest.
Arguments:
- sample_ids: int32 [4, 1024, 1024], P(None, ('grp', 'tab')), may hold values from 0 to 1535
- id_weights: bfloat16 [4, 1024, 1024], P(None, ('grp', 'tab')), may hold values from 0.25 to 2
- dense_features: bfloat16 [4, 1024, 128], P(None, ('grp', 'tab')), may hold values from -6 to 6
- click_labels: int32 [4, 1024], P(None, ('grp', 'tab')), may hold values 0 or 1
- table_shards: bfloat16 [128, 1536, 128], P('tab'), may hold values from -1.1953125 to 1.1953125
- slot_table: int32 [128], replicated, may hold values from 0 to 127, each once
- top_weight: bfloat16 [128, 1024], replicated, may hold values from -0.5 to 0.5
- top_bias: float32 [1024], replicated, may hold values from -3 to 3
- out_weight: bfloat16 [1024], replicated, may hold values from -0.1875 to 0.1875
Outputs:
- logits: float32 [4, 1024], P(None, ('grp', 'tab'))
- grad_top: float32 [128, 1024], replicated
- grad_bias: float32 [1024], replicated
The draws below stay inside these ranges and needn't reach their ends.
Inputs may be any that keep to these rules, and one draw needn't show every extreme that they name: `slot_table`: a permutation: each table stands in exactly one slot.
All inputs are finite; a program needn't handle non-finite values. No bound on the sum of `click_labels` on one device may be relied on, other than what follows from the above.
Results may differ from the reference program's by a relative error of at most 0.0056.
Values may be sent and summed in bfloat16 or wider, within the bound.
A program may use at most 128 MiB of HBM per device.

```python
import math
import jax
import jax.numpy as jnp
import numpy as np
from jax import lax

DIM = 128
VOCAB = 1536
HIDDEN_SIZE = 1024
HOTS = 8
MB = 4
TABLES = 128
BATCH = 1024


def place_ends(entries, key, smallest, largest):
    dims = entries.shape
    spot = [jax.random.randint(jax.random.fold_in(key, axis), (), 0, dims[axis]) for axis in range(len(dims))]
    entries = entries.at[tuple(spot)].set(smallest)
    longest = dims.index(max(dims))
    spot[longest] = (spot[longest] + 1) % dims[longest]
    return entries.at[tuple(spot)].set(largest)


def shard_levels(stream_key, dims, cuts, low, high):
    level, own = 1.0, jax.random.fold_in(stream_key, 6)
    for dim, blocks in cuts:
        steps = jnp.exp(jax.random.uniform(jax.random.fold_in(own, dim), (blocks,), jnp.float32, low / len(cuts), high / len(cuts)))
        level = level * jnp.repeat(steps, dims[dim] // blocks).reshape([-1 if axis == dim else 1 for axis in range(len(dims))])
    return level


def cumulative_ranks(count, lean):
    weights = [(1 << 20) // math.isqrt(standing ** lean) + 1 for standing in range(1, count + 1)]
    spread = 1 + sum(weights) // (1 << 30)
    return np.cumsum(np.array([max(1, weight // spread) for weight in weights]))


def skewed_ids(own_key, shape, number_of, skew):
    table = cumulative_ranks(number_of, skew)
    pick = jax.random.randint(jax.random.fold_in(own_key, 1), shape, 0, int(table[number_of - 1]))
    standing = jnp.searchsorted(jnp.asarray(table, jnp.int32), pick, side="right")
    return jax.random.permutation(jax.random.fold_in(own_key, 2), number_of)[standing].astype(jnp.int32)


def bell_draw(own_key, dims, width, bound, shards=(), kind=jnp.bfloat16):
    drawn = jax.random.normal(own_key, dims, jnp.float32) * width
    if len(shards) > 0:
        drawn = shard_levels(own_key, dims, shards, -0.22, 0.18) * drawn
    return jnp.clip(drawn, min=-bound, max=bound).astype(kind)


def setup_inputs(seed: int = 0) -> dict:
    key_list = jax.random.split(jax.random.key(seed), 10)
    return {
        "sample_ids": place_ends(skewed_ids(key_list[0], (MB, BATCH, TABLES * HOTS), VOCAB, 2), jax.random.fold_in(key_list[0], 3), 0, VOCAB - 1).astype(jnp.int32),
        "id_weights": jnp.clip(0.25 + 1.75 * jax.random.uniform(key_list[1], (MB, BATCH, TABLES * HOTS), jnp.float32) ** shard_levels(key_list[1], (MB, BATCH, TABLES * HOTS), ((1, 32),), -0.2, 0.2), 0.25, 2.0).astype(jnp.bfloat16),
        "dense_features": bell_draw(key_list[2], (MB, BATCH, DIM), 1.0, 6.0, ((1, 32),)),
        "click_labels": place_ends((jax.random.randint(key_list[3], (MB, BATCH), 0, 2) < 1).astype(jnp.int32), jax.random.fold_in(key_list[3], 1), 0, 1),
        "table_shards": bell_draw(key_list[4], (TABLES, VOCAB, DIM), 0.2, 1.1953125, ((0, 16),)),
        "slot_table": jax.random.permutation(key_list[5], TABLES).astype(jnp.int32),
        "top_weight": bell_draw(key_list[6], (TABLES, HIDDEN_SIZE), TABLES ** -0.5, 0.5),
        "top_bias": bell_draw(key_list[7], (HIDDEN_SIZE,), 0.5, 3.0, (), jnp.float32),
        "out_weight": bell_draw(key_list[8], (HIDDEN_SIZE,), HIDDEN_SIZE ** -0.5, 0.1875),
    }


loss_scale = 32768.0

def reference(sample_ids, id_weights, dense_features, click_labels, table_shards, slot_table, top_weight, top_bias, out_weight):
    count = MB * BATCH
    ids_all = sample_ids.reshape(count, TABLES, HOTS)
    weights_all = id_weights.reshape(count, TABLES, HOTS).astype(jnp.float32)
    features = dense_features.reshape(count, DIM).astype(jnp.float32)
    earlier = jnp.arange(HOTS)[None, :] < jnp.arange(HOTS)[:, None]
    scale = 1.0 / jnp.sqrt(jnp.float32(DIM))

    def slot_scores(slot):
        table = slot_table[slot]
        slot_ids = lax.dynamic_index_in_dim(ids_all, table, axis=1, keepdims=False)
        slot_weights = lax.dynamic_index_in_dim(weights_all, table, axis=1, keepdims=False)
        same = slot_ids[:, :, None] == slot_ids[:, None, :]
        summed = lax.optimization_barrier(jnp.sum(jnp.where(same, slot_weights[:, None, :], jnp.float32(0.0)), axis=2))
        first = jnp.logical_not(jnp.any(same & earlier[None], axis=2))
        rounded = lax.optimization_barrier(summed.astype(jnp.bfloat16)).astype(jnp.float32)
        merged = jnp.where(first, rounded, jnp.float32(0.0))
        shard = lax.dynamic_index_in_dim(table_shards, slot, axis=0, keepdims=False)
        rows = shard[slot_ids].astype(jnp.float32)
        pooled = jnp.einsum('nh,nhe->ne', merged, rows).astype(jnp.bfloat16)
        pooled_wide = lax.optimization_barrier(pooled).astype(jnp.float32)
        return (lax.optimization_barrier(jnp.sum(pooled_wide * features, axis=1)) * scale).astype(jnp.bfloat16)
    scores = lax.map(slot_scores, jnp.arange(TABLES, dtype=jnp.int32)).T
    slot_weight = top_weight[slot_table]
    pre = jnp.dot(scores, slot_weight, preferred_element_type=jnp.float32) + top_bias
    gate = jax.nn.sigmoid(pre)
    hidden = (pre * gate).astype(jnp.bfloat16)
    logit_all = jnp.dot(hidden, out_weight, preferred_element_type=jnp.float32)
    labels = click_labels.reshape(count).astype(jnp.float32)
    delta = (jax.nn.sigmoid(logit_all) - labels) * (loss_scale / count)
    slope = gate * (1.0 + pre * (1.0 - gate))
    hidden_grad = (delta[:, None] * out_weight.astype(jnp.float32)[None, :] * slope).astype(jnp.bfloat16)
    hidden_grad = lax.optimization_barrier(hidden_grad)
    grad_slot = jnp.dot(scores.T, hidden_grad, preferred_element_type=jnp.float32)
    grad_bias = lax.optimization_barrier(jnp.sum(hidden_grad.astype(jnp.float32), axis=0))
    grad_top = jnp.zeros_like(grad_slot).at[slot_table].set(grad_slot)
    return (logit_all.reshape(MB, BATCH), grad_top, grad_bias)
```

```python
import functools
import math

import jax
import jax.numpy as jnp
from jax import lax
from jax.experimental import pallas as pl
from jax.experimental.pallas import tpu as pltpu
from jax.sharding import PartitionSpec as P

HOTS = 8
LANES = 128
loss_scale = 32768.0
NT = (((1,), (1,)), ((), ()))
TN = (((0,), (0,)), ((), ()))


def score_kernel(hots, chunk, x_ref, d_ref, t_ref, o_ref, lo_ref, key_ref, acc_ref):
    slot = pl.program_id(0)
    rows = x_ref.shape[0]
    vocab = t_ref.shape[1]
    blocks = vocab // LANES
    half = x_ref.shape[1] // 2
    slots = half // hots

    @pl.when(slot == 0)
    def _():
        @pl.loop(0, rows // chunk)
        def _(c):
            at = pl.ds(c * chunk, chunk)
            code = x_ref[at, :].astype(jnp.float32)
            lane = lax.broadcasted_iota(jnp.int32, code.shape, 1)
            high = jnp.zeros(code.shape, jnp.int32)
            for k in range(1, blocks):
                high = high + (code >= float(LANES << k)).astype(jnp.int32)
            low = jnp.right_shift(code.astype(jnp.int32), high) & (LANES - 1)
            lo_ref[at, :] = low
            key_ref[at, :] = jnp.where(lane < half, (lane // hots) * blocks + high, -1)
            acc_ref[at, :] = jnp.zeros(code.shape, jnp.float32)

    @pl.loop(0, rows // chunk)
    def _(c):
        at = pl.ds(c * chunk, chunk)
        feats = d_ref[at, :]
        low = lo_ref[at, :]
        key = key_ref[at, :]
        acc = acc_ref[at, :]
        step = 2 * LANES if vocab % (2 * LANES) == 0 else LANES
        for p in range(vocab // step):
            g = lax.dot_general(feats, t_ref[0, p * step : (p + 1) * step, :], NT,
                                preferred_element_type=jnp.float32)
            for q in range(step // LANES):
                a = p * (step // LANES) + q
                part = g[:, q * LANES : (q + 1) * LANES]
                got = jnp.take_along_axis(part, low, axis=1, mode="promise_in_bounds")
                acc = jnp.where(key == slot * blocks + a, got, acc)
        acc_ref[at, :] = acc

    @pl.when(slot == slots - 1)
    def _():
        w = pltpu.roll(x_ref[...].astype(jnp.float32), half, 1)
        lane = lax.broadcasted_iota(jnp.int32, w.shape, 1)
        prod = jnp.where(lane < half, acc_ref[...] * w, 0.0)
        pick_row = lax.broadcasted_iota(jnp.int32, (slots, 2 * half), 0)
        pick_lane = lax.broadcasted_iota(jnp.int32, (slots, 2 * half), 1)
        pick = (pick_lane // hots == pick_row).astype(jnp.float32)
        total = lax.dot_general(pick, prod, NT, preferred_element_type=jnp.float32,
                                precision=lax.Precision.HIGHEST)
        o_ref[...] = (total * (1.0 / math.sqrt(d_ref.shape[1]))).astype(o_ref.dtype)


def slot_scores(x, d, table):
    rows, lanes = x.shape
    slots, vocab, width = table.shape
    hots = lanes // 2 // slots
    chunk = min(256, rows)
    return pl.pallas_call(
        functools.partial(score_kernel, hots, chunk),
        grid=(slots,),
        out_shape=jax.ShapeDtypeStruct((slots, rows), jnp.bfloat16),
        in_specs=[
            pl.BlockSpec((rows, lanes), lambda s: (0, 0)),
            pl.BlockSpec((rows, width), lambda s: (0, 0)),
            pl.BlockSpec((1, vocab, width), lambda s: (s, 0, 0)),
        ],
        out_specs=pl.BlockSpec((slots, rows), lambda s: (0, 0)),
        scratch_shapes=[
            pltpu.VMEM((rows, lanes), jnp.int32),
            pltpu.VMEM((rows, lanes), jnp.int32),
            pltpu.VMEM((rows, lanes), jnp.float32),
        ],
        cost_estimate=pl.CostEstimate(flops=2 * rows * slots * vocab * width, bytes_accessed=4 << 20,
                                      transcendentals=0),
    )(x, d, table)


def top_kernel(count, s_ref, place_ref, label_ref, w_ref, b_ref, o_ref, logit_ref, grad_ref, bias_ref):
    tables = s_ref.shape[0]
    row = lax.broadcasted_iota(jnp.int32, (tables, tables), 0)
    placed = (place_ref[...] == row).astype(jnp.bfloat16)
    scores = jnp.dot(placed, s_ref[...], preferred_element_type=jnp.float32).astype(jnp.bfloat16)
    pre = lax.dot_general(scores, w_ref[...], TN, preferred_element_type=jnp.float32) + b_ref[...]
    gate = jax.nn.sigmoid(pre)
    hidden = (pre * gate).astype(jnp.bfloat16).astype(jnp.float32)
    out = o_ref[...].astype(jnp.float32)
    logit = jnp.sum(hidden * out, axis=1, keepdims=True)
    logit_ref[...] = logit
    delta = (jax.nn.sigmoid(logit) - label_ref[...].astype(jnp.float32)) * (loss_scale / count)
    slope = gate * (1.0 + pre * (1.0 - gate))
    grad = (delta * out * slope).astype(jnp.bfloat16)
    grad_ref[...] = jnp.dot(scores, grad, preferred_element_type=jnp.float32)
    bias_ref[...] = jnp.sum(grad.astype(jnp.float32), axis=0, keepdims=True)


def top_network(count, scores, slot_table, labels, weight, bias, out):
    tables, samples = scores.shape
    hidden = weight.shape[1]
    return pl.pallas_call(
        functools.partial(top_kernel, count),
        out_shape=(
            jax.ShapeDtypeStruct((samples, 1), jnp.float32),
            jax.ShapeDtypeStruct((tables, hidden), jnp.float32),
            jax.ShapeDtypeStruct((1, hidden), jnp.float32),
        ),
    )(scores, slot_table.reshape(1, -1), labels.reshape(-1, 1), weight, bias.reshape(1, -1), out.reshape(1, -1))


def per_device(
    sample_ids, id_weights, dense_features, click_labels, table_shards, slot_table, top_weight, top_bias, out_weight
):
    micro, local_batch, columns = sample_ids.shape
    tables = slot_table.shape[0]
    slots = table_shards.shape[0]
    width = dense_features.shape[2]
    hidden = top_weight.shape[1]
    members = lax.axis_size("tab")
    groups = lax.axis_size("grp")
    samples = micro * local_batch
    count = samples * groups * members
    hots = columns // tables
    own = slots * hots

    ids = sample_ids.reshape(samples, columns)
    power = jnp.left_shift(1, ids // LANES)
    code = ((LANES + ids % LANES) * power).astype(jnp.bfloat16)
    weights = id_weights.reshape(samples, columns)
    source = (slot_table[:, None] * hots + jnp.arange(hots, dtype=jnp.int32)[None, :]).reshape(-1)
    permute = (lax.broadcasted_iota(jnp.int32, (columns, columns), 0) == source[None, :]).astype(jnp.bfloat16)
    both = jnp.dot(jnp.concatenate([code, weights], 0), permute, preferred_element_type=jnp.float32)
    both = both.astype(jnp.bfloat16)
    both = both.reshape(2, samples, members, own).transpose(2, 1, 0, 3).reshape(members * samples, 2 * own)
    x = lax.all_to_all(both, "tab", split_axis=0, concat_axis=0, tiled=True)
    d = lax.all_gather(dense_features.reshape(samples, width), "tab", axis=0, tiled=True)
    mine = slot_scores(x, d, table_shards)
    scores = lax.all_to_all(mine, "tab", split_axis=1, concat_axis=0, tiled=True)
    logit, grad, bias = top_network(
        count, scores, slot_table, click_labels.reshape(samples), top_weight, top_bias, out_weight
    )
    piece = hidden // groups
    blocks = grad.reshape(members, slots, groups, piece).transpose(2, 0, 1, 3)
    got = lax.all_to_all(blocks.reshape(groups * members, slots, piece), ("grp", "tab"), split_axis=0, concat_axis=0,
                         tiled=True)
    part = jnp.sum(got, axis=0)
    whole = lax.all_gather(part, ("grp", "tab"), axis=0, tiled=False)
    grad_top = whole.reshape(groups, members, slots, piece).transpose(1, 2, 0, 3).reshape(tables, hidden)
    bias_all = lax.all_gather(bias, ("grp", "tab"), axis=0, tiled=True)
    grad_bias = jnp.sum(bias_all, axis=0)
    return (logit.reshape(micro, local_batch), grad_top, grad_bias)


def solution(mesh):
    return jax.shard_map(
        per_device,
        mesh=mesh,
        in_specs=(
            P(None, ("grp", "tab"), None),
            P(None, ("grp", "tab"), None),
            P(None, ("grp", "tab"), None),
            P(None, ("grp", "tab")),
            P("tab", None, None),
            P(),
            P(),
            P(),
            P(),
        ),
        out_specs=(P(None, ("grp", "tab")), P(), P()),
        check_vma=False,
    )
```

```python
import functools
import math

import jax
import jax.numpy as jnp
from jax import lax
from jax.experimental import pallas as pl
from jax.experimental.pallas import tpu as pltpu
from jax.sharding import PartitionSpec as P

HOTS = 8
LANES = 128
loss_scale = 32768.0
NT = (((1,), (1,)), ((), ()))
TN = (((0,), (0,)), ((), ()))


def score_kernel(hots, chunk, x_ref, d_ref, t_ref, o_ref, lo_ref, key_ref, acc_ref):
    slot = pl.program_id(0)
    rows = x_ref.shape[0]
    vocab = t_ref.shape[1]
    blocks = vocab // LANES
    half = x_ref.shape[1] // 2
    slots = half // hots

    @pl.when(slot == 0)
    def _():
        @pl.loop(0, rows // chunk)
        def _(c):
            at = pl.ds(c * chunk, chunk)
            code = x_ref[at, :].astype(jnp.float32)
            lane = lax.broadcasted_iota(jnp.int32, code.shape, 1)
            high = jnp.zeros(code.shape, jnp.int32)
            for k in range(1, blocks):
                high = high + (code >= float(LANES << k)).astype(jnp.int32)
            low = jnp.right_shift(code.astype(jnp.int32), high) & (LANES - 1)
            lo_ref[at, :] = low
            key_ref[at, :] = jnp.where(lane < half, (lane // hots) * blocks + high, -1)
            acc_ref[at, :] = jnp.zeros(code.shape, jnp.float32)

    @pl.loop(0, rows // chunk)
    def _(c):
        at = pl.ds(c * chunk, chunk)
        feats = d_ref[at, :]
        low = lo_ref[at, :]
        key = key_ref[at, :]
        acc = acc_ref[at, :]
        step = 2 * LANES if vocab % (2 * LANES) == 0 else LANES
        for p in range(vocab // step):
            g = lax.dot_general(feats, t_ref[0, p * step : (p + 1) * step, :], NT,
                                preferred_element_type=jnp.float32)
            for q in range(step // LANES):
                a = p * (step // LANES) + q
                part = g[:, q * LANES : (q + 1) * LANES]
                got = jnp.take_along_axis(part, low, axis=1, mode="promise_in_bounds")
                acc = jnp.where(key == slot * blocks + a, got, acc)
        acc_ref[at, :] = acc

    @pl.when(slot == slots - 1)
    def _():
        w = pltpu.roll(x_ref[...].astype(jnp.float32), half, 1)
        lane = lax.broadcasted_iota(jnp.int32, w.shape, 1)
        prod = jnp.where(lane < half, acc_ref[...] * w, 0.0)
        pick_row = lax.broadcasted_iota(jnp.int32, (slots, 2 * half), 0)
        pick_lane = lax.broadcasted_iota(jnp.int32, (slots, 2 * half), 1)
        pick = (pick_lane // hots == pick_row).astype(jnp.float32)
        total = lax.dot_general(pick, prod, NT, preferred_element_type=jnp.float32,
                                precision=lax.Precision.HIGHEST)
        o_ref[...] = (total * (1.0 / math.sqrt(d_ref.shape[1]))).astype(o_ref.dtype)


def slot_scores(x, d, table):
    rows, lanes = x.shape
    slots, vocab, width = table.shape
    hots = lanes // 2 // slots
    chunk = min(256, rows)
    return pl.pallas_call(
        functools.partial(score_kernel, hots, chunk),
        grid=(slots,),
        out_shape=jax.ShapeDtypeStruct((slots, rows), jnp.bfloat16),
        in_specs=[
            pl.BlockSpec((rows, lanes), lambda s: (0, 0)),
            pl.BlockSpec((rows, width), lambda s: (0, 0)),
            pl.BlockSpec((1, vocab, width), lambda s: (s, 0, 0)),
        ],
        out_specs=pl.BlockSpec((slots, rows), lambda s: (0, 0)),
        scratch_shapes=[
            pltpu.VMEM((rows, lanes), jnp.int32),
            pltpu.VMEM((rows, lanes), jnp.int32),
            pltpu.VMEM((rows, lanes), jnp.float32),
        ],
        cost_estimate=pl.CostEstimate(flops=2 * rows * slots * vocab * width, bytes_accessed=4 << 20,
                                      transcendentals=0),
    )(x, d, table)


def top_kernel(count, s_ref, place_ref, label_ref, w_ref, b_ref, o_ref, logit_ref, grad_ref, bias_ref):
    tables = s_ref.shape[0]
    row = lax.broadcasted_iota(jnp.int32, (tables, tables), 0)
    placed = (place_ref[...] == row).astype(jnp.bfloat16)
    scores = jnp.dot(placed, s_ref[...], preferred_element_type=jnp.float32).astype(jnp.bfloat16)
    pre = lax.dot_general(scores, w_ref[...], TN, preferred_element_type=jnp.float32) + b_ref[...]
    gate = jax.nn.sigmoid(pre)
    hidden = (pre * gate).astype(jnp.bfloat16).astype(jnp.float32)
    out = o_ref[...].astype(jnp.float32)
    logit = jnp.sum(hidden * out, axis=1, keepdims=True)
    logit_ref[...] = logit
    delta = (jax.nn.sigmoid(logit) - label_ref[...].astype(jnp.float32)) * (loss_scale / count)
    slope = gate * (1.0 + pre * (1.0 - gate))
    grad = (delta * out * slope).astype(jnp.bfloat16)
    grad_ref[...] = jnp.dot(scores, grad, preferred_element_type=jnp.float32)
    bias_ref[...] = jnp.sum(grad.astype(jnp.float32), axis=0, keepdims=True)


def top_network(count, scores, slot_table, labels, weight, bias, out):
    tables, samples = scores.shape
    hidden = weight.shape[1]
    return pl.pallas_call(
        functools.partial(top_kernel, count),
        out_shape=(
            jax.ShapeDtypeStruct((samples, 1), jnp.float32),
            jax.ShapeDtypeStruct((tables, hidden), jnp.float32),
            jax.ShapeDtypeStruct((1, hidden), jnp.float32),
        ),
    )(scores, slot_table.reshape(1, -1), labels.reshape(-1, 1), weight, bias.reshape(1, -1), out.reshape(1, -1))


def spread(block, axes, count):
    copies = jnp.broadcast_to(block[None], (count,) + block.shape)
    return lax.all_to_all(copies, axes, split_axis=0, concat_axis=0, tiled=True)


def per_device(
    sample_ids, id_weights, dense_features, click_labels, table_shards, slot_table, top_weight, top_bias, out_weight
):
    micro, local_batch, columns = sample_ids.shape
    tables = slot_table.shape[0]
    slots = table_shards.shape[0]
    width = dense_features.shape[2]
    hidden = top_weight.shape[1]
    members = lax.axis_size("tab")
    groups = lax.axis_size("grp")
    samples = micro * local_batch
    count = samples * groups * members
    hots = columns // tables
    own = slots * hots

    ids = sample_ids.reshape(samples, columns)
    power = jnp.left_shift(1, ids >> (LANES.bit_length() - 1))
    code = ((LANES + (ids & (LANES - 1))) * power).astype(jnp.bfloat16)
    weights = id_weights.reshape(samples, columns)
    source = (slot_table[:, None] * hots + jnp.arange(hots, dtype=jnp.int32)[None, :]).reshape(-1)
    permute = (lax.broadcasted_iota(jnp.int32, (columns, columns), 0) == source[None, :]).astype(jnp.bfloat16)
    both = jnp.dot(jnp.concatenate([code, weights], 0), permute, preferred_element_type=jnp.float32)
    both = both.astype(jnp.bfloat16)
    both = both.reshape(2, samples, members, own).transpose(2, 1, 0, 3).reshape(members * samples, 2 * own)
    x = lax.all_to_all(both, "tab", split_axis=0, concat_axis=0, tiled=True)
    d = spread(dense_features.reshape(samples, width), "tab", members)
    d = d.reshape(members * samples, width)
    mine = slot_scores(x, d, table_shards)
    scores = lax.all_to_all(mine, "tab", split_axis=1, concat_axis=0, tiled=True)
    logit, grad, bias = top_network(
        count, scores, slot_table, click_labels.reshape(samples), top_weight, top_bias, out_weight
    )
    piece = hidden // groups
    blocks = grad.reshape(members, slots, groups, piece).transpose(2, 0, 1, 3)
    got = lax.all_to_all(blocks.reshape(groups * members, slots, piece), ("grp", "tab"), split_axis=0, concat_axis=0,
                         tiled=True)
    part = jnp.sum(got, axis=0)
    whole = spread(part, ("grp", "tab"), groups * members)
    grad_top = whole.reshape(groups, members, slots, piece).transpose(1, 2, 0, 3).reshape(tables, hidden)
    grad_bias = jnp.sum(spread(bias.reshape(-1, LANES), ("grp", "tab"), groups * members), axis=0).reshape(hidden)
    return (logit.reshape(micro, local_batch), grad_top, grad_bias)


def solution(mesh):
    return jax.shard_map(
        per_device,
        mesh=mesh,
        in_specs=(
            P(None, ("grp", "tab"), None),
            P(None, ("grp", "tab"), None),
            P(None, ("grp", "tab"), None),
            P(None, ("grp", "tab")),
            P("tab", None, None),
            P(),
            P(),
            P(),
            P(),
        ),
        out_specs=(P(None, ("grp", "tab")), P(), P()),
        check_vma=False,
    )
```

```python
import functools
import math

import jax
import jax.numpy as jnp
from jax import lax
from jax.experimental import pallas as pl
from jax.experimental.pallas import tpu as pltpu
from jax.sharding import PartitionSpec as P

HOTS = 8
LANES = 128
loss_scale = 32768.0
NT = (((1,), (1,)), ((), ()))
MESH = pl.DeviceIdType.MESH
TN = (((0,), (0,)), ((), ()))


def score_kernel(hots, chunk, x_ref, d_ref, t_ref, o_ref, lo_ref, key_ref, acc_ref, even_ref, odd_ref):
    slot = pl.program_id(0)
    rows = x_ref.shape[0]
    vocab = t_ref.shape[1]
    blocks = vocab // LANES
    half = x_ref.shape[1] // 2
    slots = half // hots
    chunks = rows // chunk
    group = 8

    @pl.when(slot == 0)
    def _():
        @pl.loop(0, chunks)
        def _(c):
            at = pl.ds(c * chunk, chunk)
            code = x_ref[at, :].astype(jnp.float32)
            lane = lax.broadcasted_iota(jnp.int32, code.shape, 1)
            high = jnp.zeros(code.shape, jnp.int32)
            for k in range(1, blocks):
                high = high + (code >= float(LANES << k)).astype(jnp.int32)
            low = jnp.right_shift(code.astype(jnp.int32), high) & (LANES - 1)
            lo_ref[at, :] = low
            key_ref[at, :] = jnp.where(lane < half, (lane // hots) * blocks + high, -1)
            acc_ref[at, :] = jnp.zeros(code.shape, jnp.float32)

    def multiply(c, g_ref):
        feats = d_ref[pl.ds(pl.multiple_of(c * chunk, chunk), chunk), :]
        step = 2 * LANES if vocab % (2 * LANES) == 0 else LANES
        for p in range(vocab // step):
            g_ref[:, p * step : (p + 1) * step] = lax.dot_general(
                feats, t_ref[0, p * step : (p + 1) * step, :], NT, preferred_element_type=jnp.float32)

    def pick(c, g_ref):
        for r in range(chunk // group):
            at = pl.ds(pl.multiple_of(c * chunk + r * group, group), group)
            low = lo_ref[at, :]
            key = key_ref[at, :] - slot * blocks
            acc = acc_ref[at, :]
            for a in range(blocks):
                part = g_ref[r * group : (r + 1) * group, a * LANES : (a + 1) * LANES]
                got = jnp.take_along_axis(part, low, axis=1, mode="promise_in_bounds")
                acc = jnp.where(key == a, got, acc)
            acc_ref[at, :] = acc

    multiply(0, even_ref)

    @pl.loop(0, chunks // 2)
    def _(i):
        multiply(2 * i + 1, odd_ref)
        pick(2 * i, even_ref)
        multiply(jnp.minimum(2 * i + 2, chunks - 1), even_ref)
        pick(2 * i + 1, odd_ref)

    @pl.when(slot == slots - 1)
    def _():
        w = pltpu.roll(x_ref[...].astype(jnp.float32), half, 1)
        lane = lax.broadcasted_iota(jnp.int32, w.shape, 1)
        prod = jnp.where(lane < half, acc_ref[...] * w, 0.0)
        pick_row = lax.broadcasted_iota(jnp.int32, (slots, 2 * half), 0)
        pick_lane = lax.broadcasted_iota(jnp.int32, (slots, 2 * half), 1)
        choose = (pick_lane // hots == pick_row).astype(jnp.float32)
        total = lax.dot_general(choose, prod, NT, preferred_element_type=jnp.float32,
                                precision=lax.Precision.HIGHEST)
        total = (total * (1.0 / math.sqrt(d_ref.shape[1]))).astype(jnp.bfloat16).astype(jnp.float32)
        samples = o_ref.shape[2]
        for m in range(o_ref.shape[0]):
            o_ref[m] = total[:, m * samples : (m + 1) * samples]


def slot_scores(x, d, table, members):
    rows, lanes = x.shape
    slots, vocab, width = table.shape
    hots = lanes // 2 // slots
    chunk = min(256, rows // 2)
    return pl.pallas_call(
        functools.partial(score_kernel, hots, chunk),
        grid=(slots,),
        out_shape=jax.ShapeDtypeStruct((members, slots, rows // members), jnp.float32),
        in_specs=[
            pl.BlockSpec((rows, lanes), lambda s: (0, 0)),
            pl.BlockSpec((rows, width), lambda s: (0, 0)),
            pl.BlockSpec((1, vocab, width), lambda s: (s, 0, 0)),
        ],
        out_specs=pl.BlockSpec((members, slots, rows // members), lambda s: (0, 0, 0)),
        scratch_shapes=[
            pltpu.VMEM((rows, lanes), jnp.int32),
            pltpu.VMEM((rows, lanes), jnp.int32),
            pltpu.VMEM((rows, lanes), jnp.float32),
            pltpu.VMEM((chunk, vocab), jnp.float32),
            pltpu.VMEM((chunk, vocab), jnp.float32),
        ],
        cost_estimate=pl.CostEstimate(flops=2 * rows * slots * vocab * width, bytes_accessed=4 << 20,
                                      transcendentals=0),
    )(x, d, table)


def column_of(row):
    size = row.shape[1]
    eye = lax.broadcasted_iota(jnp.int32, (size, size), 0) == lax.broadcasted_iota(jnp.int32, (size, size), 1)
    return jnp.sum(jnp.where(eye, row, 0.0), axis=1, keepdims=True)


def row_of(column):
    size = column.shape[0]
    eye = lax.broadcasted_iota(jnp.int32, (size, size), 0) == lax.broadcasted_iota(jnp.int32, (size, size), 1)
    return jnp.sum(jnp.where(eye, column, 0.0), axis=0, keepdims=True)


def top_kernel(count, groups, members, s_ref, place_ref, label_ref, w_ref, b_ref, o_ref,
               logit_ref, top_ref, bias_ref,
               got_ref, grad_ref, slope_ref, part_ref, sum_ref, bias_mine, bias_part,
               send1, recv1, send2, recv2, send3, recv3, send4, recv4):
    my_g, my_t = lax.axis_index("grp"), lax.axis_index("tab")
    total = groups * members
    slots = s_ref.shape[1]
    tables, samples = got_ref.shape
    hidden = w_ref.shape[1]
    piece = hidden // groups
    me = my_g * members + my_t

    def peer(k):
        p = lax.rem(me + k, total)
        return p // members, lax.rem(p, members)

    barrier = pltpu.get_barrier_semaphore()

    @pl.loop(1, total)
    def _(k):
        g, t = peer(k)
        pl.semaphore_signal(barrier, inc=1, device_id={"grp": g, "tab": t}, device_id_type=MESH)

    pl.semaphore_wait(barrier, total - 1)

    def score_copy(k):
        t = lax.rem(my_t + k, members)
        return pltpu.make_async_remote_copy(
            src_ref=s_ref.at[t], dst_ref=got_ref.at[pl.ds(pl.multiple_of(my_t * slots, slots), slots), :],
            send_sem=send1.at[k], recv_sem=recv1.at[k], device_id={"grp": my_g, "tab": t}, device_id_type=MESH)

    @pl.loop(1, members)
    def _(k):
        score_copy(k).start()

    got_ref[pl.ds(pl.multiple_of(my_t * slots, slots), slots), :] = s_ref[my_t]

    @pl.loop(1, members)
    def _(k):
        score_copy(k).wait()

    row = lax.broadcasted_iota(jnp.int32, (tables, tables), 0)
    placed = (place_ref[...] == row).astype(jnp.bfloat16)
    scores = jnp.dot(placed, got_ref[...].astype(jnp.bfloat16), preferred_element_type=jnp.float32)
    scores = scores.astype(jnp.bfloat16)
    pre = lax.dot_general(scores, w_ref[...], TN, preferred_element_type=jnp.float32) + b_ref[...]
    gate = jax.nn.sigmoid(pre)
    value = (pre * gate).astype(jnp.bfloat16).astype(jnp.float32)
    out = o_ref[...].astype(jnp.float32)
    logit = jnp.sum(value * out, axis=1, keepdims=True)
    logit_ref[...] = row_of(logit)
    delta = (jax.nn.sigmoid(logit) - column_of(label_ref[...].astype(jnp.float32))) * (loss_scale / count)
    slope = gate * (1.0 + pre * (1.0 - gate))
    slope_ref[...] = (delta * out * slope).astype(jnp.bfloat16)
    grad = slope_ref[...]
    bias = jnp.sum(grad.astype(jnp.float32), axis=0, keepdims=True)
    for i in range(hidden // LANES):
        bias_mine[i : i + 1, :] = bias[:, i * LANES : (i + 1) * LANES]
    grad_ref[...] = jnp.dot(scores, grad, preferred_element_type=jnp.float32)

    def block(g, t):
        return pl.ds(pl.multiple_of(t * slots, slots), slots), pl.ds(pl.multiple_of(g * piece, LANES), piece)

    def bias_copy(k):
        g, t = peer(k)
        return pltpu.make_async_remote_copy(
            src_ref=bias_mine, dst_ref=bias_part.at[k], send_sem=send2.at[k], recv_sem=recv2.at[k],
            device_id={"grp": g, "tab": t}, device_id_type=MESH)

    def reduce_copy(k):
        g, t = peer(k)
        r, c = block(g, t)
        return pltpu.make_async_remote_copy(
            src_ref=grad_ref.at[r, c], dst_ref=part_ref.at[k], send_sem=send3.at[k], recv_sem=recv3.at[k],
            device_id={"grp": g, "tab": t}, device_id_type=MESH)

    @pl.loop(1, total)
    def _(k):
        reduce_copy(k).start()

    @pl.loop(1, total)
    def _(k):
        bias_copy(k).start()

    r, c = block(my_g, my_t)
    part_ref[0] = grad_ref[r, c]
    bias_part[0] = bias_mine[...]

    @pl.loop(1, total)
    def _(k):
        reduce_copy(k).wait()

    sum_ref[...] = jnp.sum(part_ref[...], axis=0)
    top_ref[r, c] = sum_ref[...]

    def spread_copy(k):
        g, t = peer(k)
        return pltpu.make_async_remote_copy(
            src_ref=sum_ref, dst_ref=top_ref.at[r, c], send_sem=send4.at[k], recv_sem=recv4.at[k],
            device_id={"grp": g, "tab": t}, device_id_type=MESH)

    @pl.loop(1, total)
    def _(k):
        spread_copy(k).start()

    @pl.loop(1, total)
    def _(k):
        bias_copy(k).wait()

    def add(j, acc):
        return acc + bias_part[lax.rem(me - j + total, total)]

    bias_ref[...] = lax.fori_loop(1, total, add, bias_part[me])

    @pl.loop(1, total)
    def _(k):
        spread_copy(k).wait()


def top_network(count, groups, members, scores, slot_table, labels, weight, bias, out):
    slots, samples = scores.shape[1:]
    tables, hidden = weight.shape
    piece = hidden // groups
    total = groups * members
    rows = hidden // LANES
    vmem = pl.BlockSpec(memory_space=pltpu.VMEM)
    return pl.pallas_call(
        functools.partial(top_kernel, count, groups, members),
        out_shape=(
            jax.ShapeDtypeStruct((1, samples), jnp.float32),
            jax.ShapeDtypeStruct((tables, hidden), jnp.float32),
            jax.ShapeDtypeStruct((rows, LANES), jnp.float32),
        ),
        in_specs=[vmem] * 6,
        out_specs=(vmem,) * 3,
        scratch_shapes=[
            pltpu.VMEM((tables, samples), jnp.float32),
            pltpu.VMEM((tables, hidden), jnp.float32),
            pltpu.VMEM((samples, hidden), jnp.bfloat16),
            pltpu.VMEM((total, slots, piece), jnp.float32),
            pltpu.VMEM((slots, piece), jnp.float32),
            pltpu.VMEM((rows, LANES), jnp.float32),
            pltpu.VMEM((total, rows, LANES), jnp.float32),
        ] + [pltpu.SemaphoreType.DMA((members,))] * 2 + [pltpu.SemaphoreType.DMA((total,))] * 6,
        compiler_params=pltpu.CompilerParams(collective_id=1, has_side_effects=True),
    )(scores, slot_table.reshape(1, -1), labels.reshape(1, -1), weight, bias.reshape(1, -1), out.reshape(1, -1))


def spread(block, axes, count):
    copies = jnp.broadcast_to(block[None], (count,) + block.shape)
    return lax.all_to_all(copies, axes, split_axis=0, concat_axis=0, tiled=True)


def per_device(
    sample_ids, id_weights, dense_features, click_labels, table_shards, slot_table, top_weight, top_bias, out_weight
):
    micro, local_batch, columns = sample_ids.shape
    tables = slot_table.shape[0]
    slots = table_shards.shape[0]
    width = dense_features.shape[2]
    hidden = top_weight.shape[1]
    members = lax.axis_size("tab")
    groups = lax.axis_size("grp")
    samples = micro * local_batch
    count = samples * groups * members
    hots = columns // tables
    own = slots * hots

    ids = sample_ids.reshape(samples, columns)
    power = jnp.left_shift(1, ids >> (LANES.bit_length() - 1))
    code = ((LANES + (ids & (LANES - 1))) * power).astype(jnp.bfloat16)
    weights = id_weights.reshape(samples, columns)
    source = (slot_table[:, None] * hots + jnp.arange(hots, dtype=jnp.int32)[None, :]).reshape(-1)
    permute = (lax.broadcasted_iota(jnp.int32, (columns, columns), 0) == source[None, :]).astype(jnp.bfloat16)
    both = jnp.dot(jnp.concatenate([code, weights], 0), permute, preferred_element_type=jnp.float32)
    both = both.astype(jnp.bfloat16)
    both = both.reshape(2, samples, members, own).transpose(2, 1, 0, 3).reshape(members * samples, 2 * own)
    x = lax.all_to_all(both, "tab", split_axis=0, concat_axis=0, tiled=True)
    d = spread(dense_features.reshape(samples, width), "tab", members)
    d = d.reshape(members * samples, width)
    mine = slot_scores(x, d, table_shards, members)
    logit, grad_top, grad_bias = top_network(
        count, groups, members, mine, slot_table, click_labels.reshape(samples), top_weight, top_bias, out_weight
    )
    return (logit.reshape(micro, local_batch), grad_top, grad_bias.reshape(hidden))


def solution(mesh):
    return jax.shard_map(
        per_device,
        mesh=mesh,
        in_specs=(
            P(None, ("grp", "tab"), None),
            P(None, ("grp", "tab"), None),
            P(None, ("grp", "tab"), None),
            P(None, ("grp", "tab")),
            P("tab", None, None),
            P(),
            P(),
            P(),
            P(),
        ),
        out_specs=(P(None, ("grp", "tab")), P(), P()),
        check_vma=False,
    )
```

```python
import functools
import math

import jax
import jax.numpy as jnp
from jax import lax
from jax.experimental import pallas as pl
from jax.experimental.pallas import tpu as pltpu
from jax.sharding import PartitionSpec as P

HOTS = 8
LANES = 128
loss_scale = 32768.0
NT = (((1,), (1,)), ((), ()))
MESH = pl.DeviceIdType.MESH
TN = (((0,), (0,)), ((), ()))


def column_of(row):
    size = row.shape[1]
    eye = lax.broadcasted_iota(jnp.int32, (size, size), 0) == lax.broadcasted_iota(jnp.int32, (size, size), 1)
    return jnp.sum(jnp.where(eye, row, 0.0), axis=1, keepdims=True)


def row_of(column):
    size = column.shape[0]
    eye = lax.broadcasted_iota(jnp.int32, (size, size), 0) == lax.broadcasted_iota(jnp.int32, (size, size), 1)
    return jnp.sum(jnp.where(eye, column, 0.0), axis=0, keepdims=True)


def step_kernel(count, groups, members, x_ref, d_ref, t_ref, place_ref, label_ref, w_ref, b_ref, o_ref,
                logit_ref, top_ref, bias_ref,
                xs_ref, ds_ref, lo_ref, key_ref, acc_ref, even_ref, odd_ref, mine_ref,
                got_ref, grad_ref, slope_ref, group_ref, half_ref, part_ref, bias_part,
                x_send, x_recv, d_send, d_recv, s_send, s_recv, g_send, g_recv, p_send, p_recv,
                b_send, b_recv, a_send, a_recv, f_send, f_recv, c_send, c_recv):
    my_g, my_t = lax.axis_index("grp"), lax.axis_index("tab")
    slots, vocab, width = t_ref.shape
    samples = x_ref.shape[1]
    blocks = vocab // LANES
    half = x_ref.shape[2] // 2
    hots = half // slots
    tables = got_ref.shape[0]
    hidden = w_ref.shape[1]
    piece = hidden // groups
    per = 2 if members % 2 == 0 else 1
    chunk = per * samples
    tile = 8

    def member(k):
        return lax.rem(my_t + k, members)

    def origin(k):
        return lax.rem(my_t - k + members, members)

    def team(k):
        return lax.rem(my_g + k, groups)

    def team_origin(k):
        return lax.rem(my_g - k + groups, groups)

    def remote(src, dst, send, recv, g, t):
        return pltpu.make_async_remote_copy(src_ref=src, dst_ref=dst, send_sem=send, recv_sem=recv,
                                            device_id={"grp": g, "tab": t}, device_id_type=MESH)

    def rows_of(t):
        return pl.ds(pl.multiple_of(t * slots, slots), slots)

    def cols_of(g):
        return pl.ds(pl.multiple_of(g * piece, LANES), piece)

    barrier = pltpu.get_barrier_semaphore()

    @pl.loop(1, members)
    def _(k):
        pl.semaphore_signal(barrier, inc=1, device_id={"grp": my_g, "tab": member(k)}, device_id_type=MESH)

    @pl.loop(1, groups)
    def _(k):
        pl.semaphore_signal(barrier, inc=1, device_id={"grp": team(k), "tab": my_t}, device_id_type=MESH)

    pl.semaphore_wait(barrier, members + groups - 2)

    def x_copy(k):
        return remote(x_ref.at[member(k)], xs_ref.at[k], x_send.at[k], x_recv.at[k], my_g, member(k))

    def d_copy(k):
        return remote(d_ref, ds_ref.at[k], d_send.at[k], d_recv.at[k], my_g, member(k))

    def s_copy(k):
        return remote(mine_ref.at[k], got_ref.at[rows_of(my_t), :], s_send.at[k], s_recv.at[k], my_g, origin(k))

    @pl.loop(1, members)
    def _(k):
        d_copy(k).start()
        x_copy(k).start()

    xs_ref[0] = x_ref[my_t]
    ds_ref[0] = d_ref[...]

    pick_row = lax.broadcasted_iota(jnp.int32, (slots, 2 * half), 0)
    pick_lane = lax.broadcasted_iota(jnp.int32, (slots, 2 * half), 1)
    choose = (pick_lane // hots == pick_row).astype(jnp.float32)

    @pl.loop(0, members // per)
    def _(i):
        for e in range(per):
            @pl.when(per * i + e > 0)
            def _():
                d_copy(per * i + e).wait_recv()
                x_copy(per * i + e).wait_recv()

        for e in range(per):
            at = pl.ds(e * samples, samples)
            code = xs_ref[per * i + e].astype(jnp.float32)
            lane = lax.broadcasted_iota(jnp.int32, code.shape, 1)
            high = jnp.zeros(code.shape, jnp.int32)
            for k in range(1, blocks):
                high = high + (code >= float(LANES << k)).astype(jnp.int32)
            lo_ref[at, :] = jnp.right_shift(code.astype(jnp.int32), high) & (LANES - 1)
            key_ref[at, :] = jnp.where(lane < half, (lane // hots) * blocks + high, -1)
            acc_ref[at, :] = jnp.zeros(code.shape, jnp.float32)

        def multiply(slot, g_ref):
            feats = ds_ref[pl.ds(per * i, per)].reshape(chunk, width)
            step = 2 * LANES if vocab % (2 * LANES) == 0 else LANES
            for p in range(vocab // step):
                g_ref[:, p * step : (p + 1) * step] = lax.dot_general(
                    feats, t_ref[slot, p * step : (p + 1) * step, :], NT, preferred_element_type=jnp.float32)

        def pick(slot, g_ref):
            for r in range(chunk // tile):
                at = pl.ds(r * tile, tile)
                low = lo_ref[at, :]
                key = key_ref[at, :] - slot * blocks
                acc = acc_ref[at, :]
                for a in range(blocks):
                    part = g_ref[r * tile : (r + 1) * tile, a * LANES : (a + 1) * LANES]
                    got = jnp.take_along_axis(part, low, axis=1, mode="promise_in_bounds")
                    acc = jnp.where(key == a, got, acc)
                acc_ref[at, :] = acc

        multiply(0, even_ref)

        @pl.loop(0, slots // 2)
        def _(p):
            multiply(2 * p + 1, odd_ref)
            pick(2 * p, even_ref)
            multiply(jnp.minimum(2 * p + 2, slots - 1), even_ref)
            pick(2 * p + 1, odd_ref)

        for e in range(per):
            w = pltpu.roll(xs_ref[per * i + e].astype(jnp.float32), half, 1)
            lane = lax.broadcasted_iota(jnp.int32, w.shape, 1)
            prod = jnp.where(lane < half, acc_ref[e * samples : (e + 1) * samples, :] * w, 0.0)
            total = lax.dot_general(choose, prod, NT, preferred_element_type=jnp.float32,
                                    precision=lax.Precision.HIGHEST)
            mine_ref[per * i + e] = (total * (1.0 / math.sqrt(width))).astype(jnp.bfloat16).astype(jnp.float32)

        for e in range(per):
            @pl.when(per * i + e > 0)
            def _():
                s_copy(per * i + e).start()

    got_ref[rows_of(my_t), :] = mine_ref[0]

    @pl.loop(1, members)
    def _(k):
        d_copy(k).wait_send()
        x_copy(k).wait_send()
        s_copy(k).wait()

    row = lax.broadcasted_iota(jnp.int32, (tables, tables), 0)
    placed = (place_ref[...] == row).astype(jnp.bfloat16)
    scores = jnp.dot(placed, got_ref[...].astype(jnp.bfloat16), preferred_element_type=jnp.float32)
    scores = scores.astype(jnp.bfloat16)
    pre = lax.dot_general(scores, w_ref[...], TN, preferred_element_type=jnp.float32) + b_ref[...]
    gate = jax.nn.sigmoid(pre)
    value = (pre * gate).astype(jnp.bfloat16).astype(jnp.float32)
    out = o_ref[...].astype(jnp.float32)
    logit = jnp.sum(value * out, axis=1, keepdims=True)
    logit_ref[...] = row_of(logit)
    delta = (jax.nn.sigmoid(logit) - column_of(label_ref[...].astype(jnp.float32))) * (loss_scale / count)
    slope = gate * (1.0 + pre * (1.0 - gate))
    slope_ref[...] = (delta * out * slope).astype(jnp.bfloat16)
    grad = slope_ref[...]
    grad_ref[pl.ds(tables, 8), :] = jnp.broadcast_to(
        jnp.sum(grad.astype(jnp.float32), axis=0, keepdims=True), (8, hidden))
    grad_ref[pl.ds(0, tables), :] = jnp.dot(scores, grad, preferred_element_type=jnp.float32)

    def g_copy(k):
        return remote(grad_ref.at[:, cols_of(team(k))], group_ref.at[k], g_send.at[k], g_recv.at[k], team(k), my_t)

    @pl.loop(1, groups)
    def _(k):
        g_copy(k).start()

    half_ref[...] = grad_ref[:, cols_of(my_g)]

    @pl.loop(1, groups)
    def _(k):
        g_copy(k).wait()
        half_ref[...] += group_ref[k]

    def p_copy(k):
        return remote(half_ref.at[rows_of(member(k)), :], part_ref.at[k], p_send.at[k], p_recv.at[k], my_g, member(k))

    def b_copy(k):
        return remote(half_ref.at[pl.ds(tables, 1), :], bias_part.at[k], b_send.at[k], b_recv.at[k], my_g, member(k))

    @pl.loop(1, members)
    def _(k):
        p_copy(k).start()

    @pl.loop(1, members)
    def _(k):
        b_copy(k).start()

    part_ref[0] = half_ref[rows_of(my_t), :]
    bias_part[0] = half_ref[tables : tables + 1, :]

    @pl.loop(1, members)
    def _(k):
        p_copy(k).wait()

    own = (rows_of(my_t), cols_of(my_g))
    top_ref[own] = jnp.sum(part_ref[...], axis=0)

    def a_copy(k):
        return remote(top_ref.at[own], top_ref.at[own], a_send.at[k], a_recv.at[k], my_g, member(k))

    def f_copy(k, j):
        at = (rows_of(origin(k)), cols_of(my_g))
        return remote(top_ref.at[at], top_ref.at[at], f_send.at[j, k], f_recv.at[j, k], team(j), my_t)

    def c_copy(j):
        at = bias_ref.at[:, cols_of(my_g)]
        return remote(at, at, c_send.at[j], c_recv.at[j], team(j), my_t)

    @pl.loop(1, members)
    def _(k):
        a_copy(k).start()

    @pl.loop(1, groups)
    def _(j):
        f_copy(0, j).start()

    @pl.loop(1, members)
    def _(k):
        b_copy(k).wait()

    def add(q, total):
        return total + bias_part[lax.rem(my_t - q + members, members)]

    bias_ref[:, cols_of(my_g)] = lax.fori_loop(1, members, add, bias_part[my_t])

    @pl.loop(1, groups)
    def _(j):
        c_copy(j).start()

    @pl.loop(1, members)
    def _(k):
        a_copy(k).wait_recv()

        @pl.loop(1, groups)
        def _(j):
            f_copy(k, j).start()

    @pl.loop(1, members)
    def _(k):
        a_copy(k).wait_send()

    @pl.loop(1, groups)
    def _(j):
        c_copy(j).wait()

        @pl.loop(0, members)
        def _(k):
            f_copy(k, j).wait()


def fused_step(count, groups, members, x, d, table, slot_table, labels, weight, bias, out):
    samples, width = d.shape
    slots, vocab, _ = table.shape
    tables, hidden = weight.shape
    piece = hidden // groups
    chunk = samples * (2 if members % 2 == 0 else 1)
    lanes = x.shape[2]
    vmem = pl.BlockSpec(memory_space=pltpu.VMEM)
    f32, bf16 = jnp.float32, jnp.bfloat16
    dma = pltpu.SemaphoreType.DMA
    return pl.pallas_call(
        functools.partial(step_kernel, count, groups, members),
        out_shape=(
            jax.ShapeDtypeStruct((1, samples), f32),
            jax.ShapeDtypeStruct((tables, hidden), f32),
            jax.ShapeDtypeStruct((1, hidden), f32),
        ),
        in_specs=[vmem] * 8,
        out_specs=(vmem,) * 3,
        scratch_shapes=[
            pltpu.VMEM((members, samples, lanes), bf16),
            pltpu.VMEM((members, samples, width), bf16),
            pltpu.VMEM((chunk, lanes), jnp.int32),
            pltpu.VMEM((chunk, lanes), jnp.int32),
            pltpu.VMEM((chunk, lanes), f32),
            pltpu.VMEM((chunk, vocab), f32),
            pltpu.VMEM((chunk, vocab), f32),
            pltpu.VMEM((members, slots, samples), f32),
            pltpu.VMEM((tables, samples), f32),
            pltpu.VMEM((tables + 8, hidden), f32),
            pltpu.VMEM((samples, hidden), bf16),
            pltpu.VMEM((groups, tables + 8, piece), f32),
            pltpu.VMEM((tables + 8, piece), f32),
            pltpu.VMEM((members, slots, piece), f32),
            pltpu.VMEM((members, 1, piece), f32),
        ]
        + [dma((members,))] * 6 + [dma((groups,))] * 2 + [dma((members,))] * 6
        + [dma((groups, members))] * 2 + [dma((groups,))] * 2,
        compiler_params=pltpu.CompilerParams(collective_id=1, has_side_effects=True),
    )(x, d, table, slot_table.reshape(1, -1), labels.reshape(1, -1), weight, bias.reshape(1, -1), out.reshape(1, -1))


def per_device(
    sample_ids, id_weights, dense_features, click_labels, table_shards, slot_table, top_weight, top_bias, out_weight
):
    micro, local_batch, columns = sample_ids.shape
    tables = slot_table.shape[0]
    slots = table_shards.shape[0]
    width = dense_features.shape[2]
    hidden = top_weight.shape[1]
    members = lax.axis_size("tab")
    groups = lax.axis_size("grp")
    samples = micro * local_batch
    count = samples * groups * members
    hots = columns // tables
    own = slots * hots

    ids = sample_ids.reshape(samples, columns)
    power = jnp.left_shift(1, ids >> (LANES.bit_length() - 1))
    code = ((LANES + (ids & (LANES - 1))) * power).astype(jnp.bfloat16)
    weights = id_weights.reshape(samples, columns)
    source = (slot_table[:, None] * hots + jnp.arange(hots, dtype=jnp.int32)[None, :]).reshape(-1)
    permute = (lax.broadcasted_iota(jnp.int32, (columns, columns), 0) == source[None, :]).astype(jnp.bfloat16)
    both = jnp.dot(jnp.concatenate([code, weights], 0), permute, preferred_element_type=jnp.float32)
    both = both.astype(jnp.bfloat16)
    both = both.reshape(2, samples, members, own).transpose(2, 1, 0, 3).reshape(members, samples, 2 * own)
    logit, grad_top, grad_bias = fused_step(
        count, groups, members, both, dense_features.reshape(samples, width), table_shards, slot_table,
        click_labels.reshape(samples), top_weight, top_bias, out_weight
    )
    return (logit.reshape(micro, local_batch), grad_top, grad_bias.reshape(hidden))


def solution(mesh):
    return jax.shard_map(
        per_device,
        mesh=mesh,
        in_specs=(
            P(None, ("grp", "tab"), None),
            P(None, ("grp", "tab"), None),
            P(None, ("grp", "tab"), None),
            P(None, ("grp", "tab")),
            P("tab", None, None),
            P(),
            P(),
            P(),
            P(),
        ),
        out_specs=(P(None, ("grp", "tab")), P(), P()),
        check_vma=False,
    )
```

```python
import functools
import math

import jax
import jax.numpy as jnp
from jax import lax
from jax.experimental import pallas as pl
from jax.experimental.pallas import tpu as pltpu
from jax.sharding import PartitionSpec as P

HOTS = 8
LANES = 128
loss_scale = 32768.0
NT = (((1,), (1,)), ((), ()))
MESH = pl.DeviceIdType.MESH
TN = (((0,), (0,)), ((), ()))


def column_of(row):
    size = row.shape[1]
    eye = lax.broadcasted_iota(jnp.int32, (size, size), 0) == lax.broadcasted_iota(jnp.int32, (size, size), 1)
    return jnp.sum(jnp.where(eye, row, 0.0), axis=1, keepdims=True)


def row_of(column):
    size = column.shape[0]
    eye = lax.broadcasted_iota(jnp.int32, (size, size), 0) == lax.broadcasted_iota(jnp.int32, (size, size), 1)
    return jnp.sum(jnp.where(eye, column, 0.0), axis=0, keepdims=True)


def step_kernel(count, groups, members, id_ref, weight_ref, source_ref, d_ref, t_ref, place_ref, label_ref, w_ref, b_ref, o_ref,
                logit_ref, top_ref, bias_ref,
                x_ref, pair_ref, fin_ref, xs_ref, ds_ref, lo_ref, key_ref, acc_ref, even_ref, odd_ref, mine_ref,
                got_ref, grad_ref, slope_ref, group_ref, half_ref, part_ref, bias_part,
                x_send, x_recv, d_send, d_recv, s_send, s_recv, g_send, g_recv, p_send, p_recv,
                b_send, b_recv, a_send, a_recv, f_send, f_recv, c_send, c_recv):
    my_g, my_t = lax.axis_index("grp"), lax.axis_index("tab")
    slots, vocab, width = t_ref.shape
    samples = x_ref.shape[1]
    blocks = vocab // LANES
    half = x_ref.shape[2] // 2
    hots = half // slots
    tables = got_ref.shape[0]
    hidden = w_ref.shape[1]
    piece = hidden // groups
    per = 2 if members % 2 == 0 else 1
    chunk = per * samples
    tile = 8

    def member(k):
        return lax.rem(my_t + k, members)

    def origin(k):
        return lax.rem(my_t - k + members, members)

    def team(k):
        return lax.rem(my_g + k, groups)

    def team_origin(k):
        return lax.rem(my_g - k + groups, groups)

    def remote(src, dst, send, recv, g, t):
        return pltpu.make_async_remote_copy(src_ref=src, dst_ref=dst, send_sem=send, recv_sem=recv,
                                            device_id={"grp": g, "tab": t}, device_id_type=MESH)

    def rows_of(t):
        return pl.ds(pl.multiple_of(t * slots, slots), slots)

    def cols_of(g):
        return pl.ds(pl.multiple_of(g * piece, LANES), piece)

    barrier = pltpu.get_barrier_semaphore()

    @pl.loop(1, members)
    def _(k):
        pl.semaphore_signal(barrier, inc=1, device_id={"grp": my_g, "tab": member(k)}, device_id_type=MESH)

    @pl.loop(1, groups)
    def _(k):
        pl.semaphore_signal(barrier, inc=1, device_id={"grp": team(k), "tab": my_t}, device_id_type=MESH)

    columns = id_ref.shape[2]
    ids = id_ref[...].reshape(samples, columns)
    code = jnp.left_shift(LANES + (ids & (LANES - 1)), jnp.right_shift(ids, LANES.bit_length() - 1))
    pair_ref[:, 0:columns] = code.astype(jnp.float32).astype(jnp.bfloat16)
    pair_ref[:, columns : 2 * columns] = weight_ref[...].reshape(samples, columns)

    @pl.loop(0, members)
    def _(m):
        spot = lax.broadcasted_iota(jnp.int32, (2 * columns, 2 * half), 0)
        chosen = (spot == source_ref[m]).astype(jnp.float32).astype(jnp.bfloat16)
        x_ref[m] = jnp.dot(pair_ref[...], chosen, preferred_element_type=jnp.float32).astype(jnp.bfloat16)

    pl.semaphore_wait(barrier, members + groups - 2)

    def x_copy(k):
        return remote(x_ref.at[member(k)], xs_ref.at[k], x_send.at[k], x_recv.at[k], my_g, member(k))

    def d_copy(k):
        return remote(d_ref, ds_ref.at[k], d_send.at[k], d_recv.at[k], my_g, member(k))

    def s_copy(k):
        return remote(mine_ref.at[k], got_ref.at[rows_of(my_t), :], s_send.at[k], s_recv.at[k], my_g, origin(k))

    @pl.loop(1, members)
    def _(k):
        d_copy(k).start()
        x_copy(k).start()

    xs_ref[0] = x_ref[my_t]
    ds_ref[0] = d_ref[...]

    pick_row = lax.broadcasted_iota(jnp.int32, (slots, 2 * half), 0)
    pick_lane = lax.broadcasted_iota(jnp.int32, (slots, 2 * half), 1)
    choose = (pick_lane // hots == pick_row).astype(jnp.float32)

    @pl.loop(0, members // per)
    def _(i):
        for e in range(per):
            @pl.when(per * i + e > 0)
            def _():
                d_copy(per * i + e).wait_recv()
                x_copy(per * i + e).wait_recv()

        for e in range(per):
            at = pl.ds(e * samples, samples)
            code = xs_ref[per * i + e].astype(jnp.float32)
            lane = lax.broadcasted_iota(jnp.int32, code.shape, 1)
            high = jnp.zeros(code.shape, jnp.int32)
            for k in range(1, blocks):
                high = high + (code >= float(LANES << k)).astype(jnp.int32)
            lo_ref[at, :] = jnp.right_shift(code.astype(jnp.int32), high) & (LANES - 1)
            key_ref[at, :] = jnp.where(lane < half, (lane // hots) * blocks + high, -1)
            acc_ref[at, :] = jnp.zeros(code.shape, jnp.float32)

        def multiply(slot, g_ref):
            feats = ds_ref[pl.ds(per * i, per)].reshape(chunk, width)
            step = 2 * LANES if vocab % (2 * LANES) == 0 else LANES
            for p in range(vocab // step):
                g_ref[:, p * step : (p + 1) * step] = lax.dot_general(
                    feats, t_ref[slot, p * step : (p + 1) * step, :], NT, preferred_element_type=jnp.float32)

        def pick(slot, g_ref):
            for r in range(chunk // tile):
                at = pl.ds(r * tile, tile)
                low = lo_ref[at, :]
                key = key_ref[at, :] - slot * blocks
                acc = acc_ref[at, :]
                for a in range(blocks):
                    part = g_ref[r * tile : (r + 1) * tile, a * LANES : (a + 1) * LANES]
                    got = jnp.take_along_axis(part, low, axis=1, mode="promise_in_bounds")
                    acc = jnp.where(key == a, got, acc)
                acc_ref[at, :] = acc

        multiply(0, even_ref)

        @pl.loop(0, slots // 2)
        def _(p):
            multiply(2 * p + 1, odd_ref)
            pick(2 * p, even_ref)
            multiply(jnp.minimum(2 * p + 2, slots - 1), even_ref)
            pick(2 * p + 1, odd_ref)

        for e in range(per):
            w = pltpu.roll(xs_ref[per * i + e].astype(jnp.float32), half, 1)
            lane = lax.broadcasted_iota(jnp.int32, w.shape, 1)
            prod = jnp.where(lane < half, acc_ref[e * samples : (e + 1) * samples, :] * w, 0.0)
            total = lax.dot_general(choose, prod, NT, preferred_element_type=jnp.float32,
                                    precision=lax.Precision.HIGHEST)
            mine_ref[per * i + e] = (total * (1.0 / math.sqrt(width))).astype(jnp.bfloat16).astype(jnp.float32)

        for e in range(per):
            @pl.when(per * i + e > 0)
            def _():
                s_copy(per * i + e).start()

    got_ref[rows_of(my_t), :] = mine_ref[0]

    @pl.loop(1, members)
    def _(k):
        d_copy(k).wait_send()
        x_copy(k).wait_send()
        s_copy(k).wait()

    row = lax.broadcasted_iota(jnp.int32, (tables, tables), 0)
    placed = (place_ref[...] == row).astype(jnp.bfloat16)
    scores = jnp.dot(placed, got_ref[...].astype(jnp.bfloat16), preferred_element_type=jnp.float32)
    scores = scores.astype(jnp.bfloat16)
    pre = lax.dot_general(scores, w_ref[...], TN, preferred_element_type=jnp.float32) + b_ref[...]
    gate = jax.nn.sigmoid(pre)
    value = (pre * gate).astype(jnp.bfloat16).astype(jnp.float32)
    out = o_ref[...].astype(jnp.float32)
    logit = jnp.sum(value * out, axis=1, keepdims=True)
    logit_row = row_of(logit)
    micro, local = logit_ref.shape
    for m in range(micro):
        logit_ref[m : m + 1, :] = logit_row[:, m * local : (m + 1) * local]
    labels = jnp.concatenate([label_ref[m : m + 1, :].astype(jnp.float32) for m in range(micro)], axis=1)
    delta = (jax.nn.sigmoid(logit) - column_of(labels)) * (loss_scale / count)
    slope = gate * (1.0 + pre * (1.0 - gate))
    slope_ref[...] = (delta * out * slope).astype(jnp.bfloat16)
    grad = slope_ref[...]
    grad_ref[pl.ds(tables, 8), :] = jnp.broadcast_to(
        jnp.sum(grad.astype(jnp.float32), axis=0, keepdims=True), (8, hidden))
    grad_ref[pl.ds(0, tables), :] = jnp.dot(scores, grad, preferred_element_type=jnp.float32)

    def g_copy(k):
        return remote(grad_ref.at[:, cols_of(team(k))], group_ref.at[k], g_send.at[k], g_recv.at[k], team(k), my_t)

    @pl.loop(1, groups)
    def _(k):
        g_copy(k).start()

    half_ref[...] = grad_ref[:, cols_of(my_g)]

    @pl.loop(1, groups)
    def _(k):
        g_copy(k).wait()
        half_ref[...] += group_ref[k]

    def p_copy(k):
        return remote(half_ref.at[rows_of(member(k)), :], part_ref.at[k], p_send.at[k], p_recv.at[k], my_g, member(k))

    def b_copy(k):
        return remote(half_ref.at[pl.ds(tables, 1), :], bias_part.at[k], b_send.at[k], b_recv.at[k], my_g, member(k))

    @pl.loop(1, members)
    def _(k):
        p_copy(k).start()

    @pl.loop(1, members)
    def _(k):
        b_copy(k).start()

    part_ref[0] = half_ref[rows_of(my_t), :]
    bias_part[0] = half_ref[tables : tables + 1, :]

    @pl.loop(1, members)
    def _(k):
        p_copy(k).wait()

    fin_ref[my_t, :, cols_of(my_g)] = jnp.sum(part_ref[...], axis=0).astype(jnp.bfloat16)

    def a_copy(k):
        at = fin_ref.at[my_t, :, cols_of(my_g)]
        return remote(at, at, a_send.at[k], a_recv.at[k], my_g, member(k))

    def f_copy(k, j):
        at = fin_ref.at[origin(k), :, cols_of(my_g)]
        return remote(at, at, f_send.at[j, k], f_recv.at[j, k], team(j), my_t)

    def c_copy(j):
        at = bias_ref.at[:, cols_of(my_g)]
        return remote(at, at, c_send.at[j], c_recv.at[j], team(j), my_t)

    @pl.loop(1, members)
    def _(k):
        a_copy(k).start()

    @pl.loop(1, groups)
    def _(j):
        f_copy(0, j).start()

    @pl.loop(1, members)
    def _(k):
        b_copy(k).wait()

    def add(q, total):
        return total + bias_part[lax.rem(my_t - q + members, members)]

    bias_ref[:, cols_of(my_g)] = lax.fori_loop(1, members, add, bias_part[my_t])

    @pl.loop(1, groups)
    def _(j):
        c_copy(j).start()

    @pl.loop(1, members)
    def _(k):
        a_copy(k).wait_recv()

        @pl.loop(1, groups)
        def _(j):
            f_copy(k, j).start()

    @pl.loop(1, members)
    def _(k):
        a_copy(k).wait_send()

    @pl.loop(1, groups)
    def _(j):
        c_copy(j).wait()

        @pl.loop(0, members)
        def _(k):
            f_copy(k, j).wait()

    for m in range(members):
        top_ref[m * slots : (m + 1) * slots, :] = fin_ref[m].astype(jnp.float32)


def fused_step(count, groups, members, ids, id_weights, source, d, table, slot_table, labels, weight, bias, out):
    samples, width = d.shape
    slots, vocab, _ = table.shape
    tables, hidden = weight.shape
    piece = hidden // groups
    chunk = samples * (2 if members % 2 == 0 else 1)
    lanes = source.shape[2]
    columns = ids.shape[2]
    vmem = pl.BlockSpec(memory_space=pltpu.VMEM)
    f32, bf16 = jnp.float32, jnp.bfloat16
    dma = pltpu.SemaphoreType.DMA
    return pl.pallas_call(
        functools.partial(step_kernel, count, groups, members),
        out_shape=(
            jax.ShapeDtypeStruct(labels.shape, f32),
            jax.ShapeDtypeStruct((tables, hidden), f32),
            jax.ShapeDtypeStruct((1, hidden), f32),
        ),
        in_specs=[vmem] * 10,
        out_specs=(vmem,) * 3,
        scratch_shapes=[
            pltpu.VMEM((members, samples, lanes), bf16),
            pltpu.VMEM((samples, 2 * columns), bf16),
            pltpu.VMEM((members, slots, hidden), bf16),
            pltpu.VMEM((members, samples, lanes), bf16),
            pltpu.VMEM((members, samples, width), bf16),
            pltpu.VMEM((chunk, lanes), jnp.int32),
            pltpu.VMEM((chunk, lanes), jnp.int32),
            pltpu.VMEM((chunk, lanes), f32),
            pltpu.VMEM((chunk, vocab), f32),
            pltpu.VMEM((chunk, vocab), f32),
            pltpu.VMEM((members, slots, samples), f32),
            pltpu.VMEM((tables, samples), f32),
            pltpu.VMEM((tables + 8, hidden), f32),
            pltpu.VMEM((samples, hidden), bf16),
            pltpu.VMEM((groups, tables + 8, piece), f32),
            pltpu.VMEM((tables + 8, piece), f32),
            pltpu.VMEM((members, slots, piece), f32),
            pltpu.VMEM((members, 1, piece), f32),
        ]
        + [dma((members,))] * 6 + [dma((groups,))] * 2 + [dma((members,))] * 6
        + [dma((groups, members))] * 2 + [dma((groups,))] * 2,
        compiler_params=pltpu.CompilerParams(collective_id=1, has_side_effects=True),
    )(ids, id_weights, source, d, table, slot_table.reshape(1, -1), labels, weight, bias.reshape(1, -1), out.reshape(1, -1))


def per_device(
    sample_ids, id_weights, dense_features, click_labels, table_shards, slot_table, top_weight, top_bias, out_weight
):
    micro, local_batch, columns = sample_ids.shape
    tables = slot_table.shape[0]
    slots = table_shards.shape[0]
    width = dense_features.shape[2]
    hidden = top_weight.shape[1]
    members = lax.axis_size("tab")
    groups = lax.axis_size("grp")
    samples = micro * local_batch
    count = samples * groups * members
    hots = columns // tables
    own = slots * hots

    source = slot_table.reshape(members, slots, 1) * hots + jnp.arange(hots, dtype=jnp.int32)
    source = source.reshape(members, 1, own)
    source = jnp.concatenate([source, source + columns], axis=2)
    logit, grad_top, grad_bias = fused_step(
        count, groups, members, sample_ids, id_weights, source, dense_features.reshape(samples, width), table_shards,
        slot_table, click_labels, top_weight, top_bias, out_weight
    )
    return (logit, grad_top, grad_bias.reshape(hidden))


def solution(mesh):
    return jax.shard_map(
        per_device,
        mesh=mesh,
        in_specs=(
            P(None, ("grp", "tab"), None),
            P(None, ("grp", "tab"), None),
            P(None, ("grp", "tab"), None),
            P(None, ("grp", "tab")),
            P("tab", None, None),
            P(),
            P(),
            P(),
            P(),
        ),
        out_specs=(P(None, ("grp", "tab")), P(), P()),
        check_vma=False,
    )
```

```python
import functools
import math

import jax
import jax.numpy as jnp
from jax import lax
from jax.experimental import pallas as pl
from jax.experimental.pallas import tpu as pltpu
from jax.sharding import PartitionSpec as P

HOTS = 8
LANES = 128
loss_scale = 32768.0
NT = (((1,), (1,)), ((), ()))
MESH = pl.DeviceIdType.MESH
TN = (((0,), (0,)), ((), ()))


def column_of(row):
    size = row.shape[1]
    eye = lax.broadcasted_iota(jnp.int32, (size, size), 0) == lax.broadcasted_iota(jnp.int32, (size, size), 1)
    return jnp.sum(jnp.where(eye, row, 0.0), axis=1, keepdims=True)


def row_of(column):
    size = column.shape[0]
    eye = lax.broadcasted_iota(jnp.int32, (size, size), 0) == lax.broadcasted_iota(jnp.int32, (size, size), 1)
    return jnp.sum(jnp.where(eye, column, 0.0), axis=0, keepdims=True)


def step_kernel(count, groups, members, id_ref, weight_ref, source_ref, d_ref, t_ref, place_ref, label_ref, w_ref, b_ref, o_ref,
                logit_ref, top_ref, bias_ref,
                turned_ref, x_ref, pair_ref, fin_ref, xs_ref, ds_ref, lo_ref, key_ref, acc_ref, even_ref, odd_ref, mine_ref,
                got_ref, grad_ref, slope_ref, group_ref, half_ref, part_ref, bias_part,
                x_send, x_recv, d_send, d_recv, s_send, s_recv, g_send, g_recv, p_send, p_recv,
                b_send, b_recv, a_send, a_recv, f_send, f_recv, c_send, c_recv):
    my_g, my_t = lax.axis_index("grp"), lax.axis_index("tab")
    slots, vocab, width = t_ref.shape
    samples = x_ref.shape[1]
    blocks = vocab // LANES
    half = x_ref.shape[2] // 2
    hots = half // slots
    tables = got_ref.shape[0]
    hidden = w_ref.shape[1]
    piece = hidden // groups
    per = 2 if members % 2 == 0 else 1
    chunk = per * samples
    tile = 8

    def member(k):
        return lax.rem(my_t + k, members)

    def origin(k):
        return lax.rem(my_t - k + members, members)

    def team(k):
        return lax.rem(my_g + k, groups)

    def team_origin(k):
        return lax.rem(my_g - k + groups, groups)

    def remote(src, dst, send, recv, g, t):
        return pltpu.make_async_remote_copy(src_ref=src, dst_ref=dst, send_sem=send, recv_sem=recv,
                                            device_id={"grp": g, "tab": t}, device_id_type=MESH)

    def rows_of(t):
        return pl.ds(pl.multiple_of(t * slots, slots), slots)

    def cols_of(g):
        return pl.ds(pl.multiple_of(g * piece, LANES), piece)

    barrier = pltpu.get_barrier_semaphore()

    @pl.loop(1, members)
    def _(k):
        pl.semaphore_signal(barrier, inc=1, device_id={"grp": my_g, "tab": member(k)}, device_id_type=MESH)

    @pl.loop(1, groups)
    def _(k):
        pl.semaphore_signal(barrier, inc=1, device_id={"grp": team(k), "tab": my_t}, device_id_type=MESH)

    columns = id_ref.shape[2]
    ids = id_ref[...].reshape(samples, columns)
    code = jnp.left_shift(LANES + (ids & (LANES - 1)), jnp.right_shift(ids, LANES.bit_length() - 1))
    pair_ref[:, 0:columns] = code.astype(jnp.float32).astype(jnp.bfloat16)
    pair_ref[:, columns : 2 * columns] = weight_ref[...].reshape(samples, columns)

    @pl.loop(0, members)
    def _(m):
        spot = lax.broadcasted_iota(jnp.int32, (2 * columns, 2 * half), 0)
        chosen = (spot == source_ref[m]).astype(jnp.float32).astype(jnp.bfloat16)
        x_ref[m] = jnp.dot(pair_ref[...], chosen, preferred_element_type=jnp.float32).astype(jnp.bfloat16)

    pl.semaphore_wait(barrier, members + groups - 2)

    def x_copy(k):
        return remote(x_ref.at[member(k)], xs_ref.at[k], x_send.at[k], x_recv.at[k], my_g, member(k))

    def d_copy(k):
        return remote(d_ref, ds_ref.at[k], d_send.at[k], d_recv.at[k], my_g, member(k))

    def s_copy(k):
        return remote(mine_ref.at[k], got_ref.at[rows_of(my_t), :], s_send.at[k], s_recv.at[k], my_g, origin(k))

    @pl.loop(1, members)
    def _(k):
        d_copy(k).start()
        x_copy(k).start()

    xs_ref[0] = x_ref[my_t]
    ds_ref[0] = d_ref[...]

    @pl.loop(0, slots)
    def _(slot):
        turned_ref[slot] = t_ref[slot].T

    pick_row = lax.broadcasted_iota(jnp.int32, (slots, 2 * half), 0)
    pick_lane = lax.broadcasted_iota(jnp.int32, (slots, 2 * half), 1)
    choose = (pick_lane // hots == pick_row).astype(jnp.float32)

    @pl.loop(0, members // per)
    def _(i):
        for e in range(per):
            @pl.when(per * i + e > 0)
            def _():
                d_copy(per * i + e).wait_recv()
                x_copy(per * i + e).wait_recv()

        for e in range(per):
            at = pl.ds(e * samples, samples)
            code = xs_ref[per * i + e].astype(jnp.float32)
            lane = lax.broadcasted_iota(jnp.int32, code.shape, 1)
            high = jnp.zeros(code.shape, jnp.int32)
            for k in range(1, blocks):
                high = high + (code >= float(LANES << k)).astype(jnp.int32)
            lo_ref[at, :] = jnp.right_shift(code.astype(jnp.int32), high) & (LANES - 1)
            key_ref[at, :] = jnp.where(lane < half, (lane // hots) * blocks + high, -1)
            acc_ref[at, :] = jnp.zeros(code.shape, jnp.float32)

        def multiply(slot, g_ref):
            feats = ds_ref[pl.ds(per * i, per)].reshape(chunk, width)
            step = 2 * LANES if vocab % (2 * LANES) == 0 else LANES
            for p in range(vocab // step):
                g_ref[:, p * step : (p + 1) * step] = jnp.dot(
                    feats, turned_ref[slot, :, p * step : (p + 1) * step], preferred_element_type=jnp.float32)

        def pick(slot, g_ref):
            for r in range(chunk // tile):
                at = pl.ds(r * tile, tile)
                low = lo_ref[at, :]
                key = key_ref[at, :] - slot * blocks
                acc = acc_ref[at, :]
                for a in range(blocks):
                    part = g_ref[r * tile : (r + 1) * tile, a * LANES : (a + 1) * LANES]
                    got = jnp.take_along_axis(part, low, axis=1, mode="promise_in_bounds")
                    acc = jnp.where(key == a, got, acc)
                acc_ref[at, :] = acc

        multiply(0, even_ref)

        @pl.loop(0, slots // 2)
        def _(p):
            multiply(2 * p + 1, odd_ref)
            pick(2 * p, even_ref)
            multiply(jnp.minimum(2 * p + 2, slots - 1), even_ref)
            pick(2 * p + 1, odd_ref)

        for e in range(per):
            w = pltpu.roll(xs_ref[per * i + e].astype(jnp.float32), half, 1)
            lane = lax.broadcasted_iota(jnp.int32, w.shape, 1)
            prod = jnp.where(lane < half, acc_ref[e * samples : (e + 1) * samples, :] * w, 0.0)
            total = lax.dot_general(choose, prod, NT, preferred_element_type=jnp.float32,
                                    precision=lax.Precision.HIGHEST)
            mine_ref[per * i + e] = (total * (1.0 / math.sqrt(width))).astype(jnp.bfloat16).astype(jnp.float32)

        for e in range(per):
            @pl.when(per * i + e > 0)
            def _():
                s_copy(per * i + e).start()

    got_ref[rows_of(my_t), :] = mine_ref[0]

    @pl.loop(1, members)
    def _(k):
        d_copy(k).wait_send()
        x_copy(k).wait_send()
        s_copy(k).wait()

    row = lax.broadcasted_iota(jnp.int32, (tables, tables), 0)
    placed = (place_ref[...] == row).astype(jnp.bfloat16)
    scores = jnp.dot(placed, got_ref[...].astype(jnp.bfloat16), preferred_element_type=jnp.float32)
    scores = scores.astype(jnp.bfloat16)
    pre = lax.dot_general(scores, w_ref[...], TN, preferred_element_type=jnp.float32) + b_ref[...]
    gate = jax.nn.sigmoid(pre)
    value = (pre * gate).astype(jnp.bfloat16).astype(jnp.float32)
    out = o_ref[...].astype(jnp.float32)
    logit = jnp.sum(value * out, axis=1, keepdims=True)
    logit_row = row_of(logit)
    micro, local = logit_ref.shape
    for m in range(micro):
        logit_ref[m : m + 1, :] = logit_row[:, m * local : (m + 1) * local]
    labels = jnp.concatenate([label_ref[m : m + 1, :].astype(jnp.float32) for m in range(micro)], axis=1)
    delta = (jax.nn.sigmoid(logit) - column_of(labels)) * (loss_scale / count)
    slope = gate * (1.0 + pre * (1.0 - gate))
    slope_ref[...] = (delta * out * slope).astype(jnp.bfloat16)
    grad = slope_ref[...]
    grad_ref[pl.ds(tables, 8), :] = jnp.broadcast_to(
        jnp.sum(grad.astype(jnp.float32), axis=0, keepdims=True), (8, hidden))
    grad_ref[pl.ds(0, tables), :] = jnp.dot(scores, grad, preferred_element_type=jnp.float32)

    def g_copy(k):
        return remote(grad_ref.at[:, cols_of(team(k))], group_ref.at[k], g_send.at[k], g_recv.at[k], team(k), my_t)

    @pl.loop(1, groups)
    def _(k):
        g_copy(k).start()

    half_ref[...] = grad_ref[:, cols_of(my_g)]

    @pl.loop(1, groups)
    def _(k):
        g_copy(k).wait()
        half_ref[...] += group_ref[k]

    def p_copy(k):
        return remote(half_ref.at[rows_of(member(k)), :], part_ref.at[k], p_send.at[k], p_recv.at[k], my_g, member(k))

    def b_copy(k):
        return remote(half_ref.at[pl.ds(tables, 1), :], bias_part.at[k], b_send.at[k], b_recv.at[k], my_g, member(k))

    @pl.loop(1, members)
    def _(k):
        p_copy(k).start()

    @pl.loop(1, members)
    def _(k):
        b_copy(k).start()

    part_ref[0] = half_ref[rows_of(my_t), :]
    bias_part[0] = half_ref[tables : tables + 1, :]

    @pl.loop(1, members)
    def _(k):
        p_copy(k).wait()

    fin_ref[my_t, :, cols_of(my_g)] = jnp.sum(part_ref[...], axis=0).astype(jnp.bfloat16)

    def a_copy(k):
        at = fin_ref.at[my_t, :, cols_of(my_g)]
        return remote(at, at, a_send.at[k], a_recv.at[k], my_g, member(k))

    def f_copy(k, j):
        at = fin_ref.at[origin(k), :, cols_of(my_g)]
        return remote(at, at, f_send.at[j, k], f_recv.at[j, k], team(j), my_t)

    def c_copy(j):
        at = bias_ref.at[:, cols_of(my_g)]
        return remote(at, at, c_send.at[j], c_recv.at[j], team(j), my_t)

    @pl.loop(1, members)
    def _(k):
        a_copy(k).start()

    @pl.loop(1, groups)
    def _(j):
        f_copy(0, j).start()

    @pl.loop(1, members)
    def _(k):
        b_copy(k).wait()

    def add(q, total):
        return total + bias_part[lax.rem(my_t - q + members, members)]

    bias_ref[:, cols_of(my_g)] = lax.fori_loop(1, members, add, bias_part[my_t])

    @pl.loop(1, groups)
    def _(j):
        c_copy(j).start()

    @pl.loop(1, members)
    def _(k):
        a_copy(k).wait_recv()

        @pl.loop(1, groups)
        def _(j):
            f_copy(k, j).start()

    @pl.loop(1, members)
    def _(k):
        a_copy(k).wait_send()

    @pl.loop(1, groups)
    def _(j):
        c_copy(j).wait()

        @pl.loop(0, members)
        def _(k):
            f_copy(k, j).wait()

    for m in range(members):
        top_ref[m * slots : (m + 1) * slots, :] = fin_ref[m].astype(jnp.float32)


def fused_step(count, groups, members, ids, id_weights, source, d, table, slot_table, labels, weight, bias, out):
    samples, width = d.shape
    slots, vocab, _ = table.shape
    tables, hidden = weight.shape
    piece = hidden // groups
    chunk = samples * (2 if members % 2 == 0 else 1)
    lanes = source.shape[2]
    columns = ids.shape[2]
    vmem = pl.BlockSpec(memory_space=pltpu.VMEM)
    f32, bf16 = jnp.float32, jnp.bfloat16
    dma = pltpu.SemaphoreType.DMA
    return pl.pallas_call(
        functools.partial(step_kernel, count, groups, members),
        out_shape=(
            jax.ShapeDtypeStruct(labels.shape, f32),
            jax.ShapeDtypeStruct((tables, hidden), f32),
            jax.ShapeDtypeStruct((1, hidden), f32),
        ),
        in_specs=[vmem] * 10,
        out_specs=(vmem,) * 3,
        scratch_shapes=[
            pltpu.VMEM((slots, width, vocab), bf16),
            pltpu.VMEM((members, samples, lanes), bf16),
            pltpu.VMEM((samples, 2 * columns), bf16),
            pltpu.VMEM((members, slots, hidden), bf16),
            pltpu.VMEM((members, samples, lanes), bf16),
            pltpu.VMEM((members, samples, width), bf16),
            pltpu.VMEM((chunk, lanes), jnp.int32),
            pltpu.VMEM((chunk, lanes), jnp.int32),
            pltpu.VMEM((chunk, lanes), f32),
            pltpu.VMEM((chunk, vocab), f32),
            pltpu.VMEM((chunk, vocab), f32),
            pltpu.VMEM((members, slots, samples), f32),
            pltpu.VMEM((tables, samples), f32),
            pltpu.VMEM((tables + 8, hidden), f32),
            pltpu.VMEM((samples, hidden), bf16),
            pltpu.VMEM((groups, tables + 8, piece), f32),
            pltpu.VMEM((tables + 8, piece), f32),
            pltpu.VMEM((members, slots, piece), f32),
            pltpu.VMEM((members, 1, piece), f32),
        ]
        + [dma((members,))] * 6 + [dma((groups,))] * 2 + [dma((members,))] * 6
        + [dma((groups, members))] * 2 + [dma((groups,))] * 2,
        compiler_params=pltpu.CompilerParams(collective_id=1, has_side_effects=True),
    )(ids, id_weights, source, d, table, slot_table.reshape(1, -1), labels, weight, bias.reshape(1, -1), out.reshape(1, -1))


def per_device(
    sample_ids, id_weights, dense_features, click_labels, table_shards, slot_table, top_weight, top_bias, out_weight
):
    micro, local_batch, columns = sample_ids.shape
    tables = slot_table.shape[0]
    slots = table_shards.shape[0]
    width = dense_features.shape[2]
    hidden = top_weight.shape[1]
    members = lax.axis_size("tab")
    groups = lax.axis_size("grp")
    samples = micro * local_batch
    count = samples * groups * members
    hots = columns // tables
    own = slots * hots

    source = slot_table.reshape(members, slots, 1) * hots + jnp.arange(hots, dtype=jnp.int32)
    source = source.reshape(members, 1, own)
    source = jnp.concatenate([source, source + columns], axis=2)
    logit, grad_top, grad_bias = fused_step(
        count, groups, members, sample_ids, id_weights, source, dense_features.reshape(samples, width), table_shards,
        slot_table, click_labels, top_weight, top_bias, out_weight
    )
    return (logit, grad_top, grad_bias.reshape(hidden))


def solution(mesh):
    return jax.shard_map(
        per_device,
        mesh=mesh,
        in_specs=(
            P(None, ("grp", "tab"), None),
            P(None, ("grp", "tab"), None),
            P(None, ("grp", "tab"), None),
            P(None, ("grp", "tab")),
            P("tab", None, None),
            P(),
            P(),
            P(),
            P(),
        ),
        out_specs=(P(None, ("grp", "tab")), P(), P()),
        check_vma=False,
    )
```
